512 devices in a mesh: ma: 64 (over z, x, core), ba: 8 (over y).
Axes of the slice: x: 4, y: 8, z: 8, core: 2. Of those that a mesh axis runs over, the one named last changes fastest.
Arguments:
- fields: bfloat16 [16, 256, 256, 192], P('ba', 'ma'), may hold values from -6 to 6
- weight_real: bfloat16 [112, 64, 192, 192], P('ba', 'ma'), may hold values from -0.4375 to 0.4375
- weight_imag: bfloat16 [112, 64, 192, 192], P('ba', 'ma'), may hold values from -0.4375 to 0.4375
- skip_weight: bfloat16 [192, 192], replicated, may hold values from -0.4375 to 0.4375
- out_bias: float32 [192], replicated, may hold values from -3 to 3
Outputs:
- layer_out: bfloat16 [16, 256, 256, 192], P('ba', 'ma')
The draws below stay inside these ranges and needn't reach their ends.
All inputs are finite; a program needn't handle non-finite values.
Results may differ from the reference program's by a relative error of at most 0.0095.
Values may be sent and summed in bfloat16 or wider, within the bound.
A program may use at most 64 MiB of HBM per device.

```python
import math
import jax
import jax.numpy as jnp
from jax import lax

C = 192
H = 256
W = 256
KX = 112
KY = 64
B = 16


def shard_levels(own_key, dims, cuts, low, largest):
    def one(dim, parts):
        heights = jax.random.uniform(jax.random.fold_in(jax.random.fold_in(own_key, 6), dim), (parts,), jnp.float32, low / len(cuts), largest / len(cuts))
        return jnp.repeat(jnp.exp(heights), dims[dim] // parts).reshape((-1,) + (1,) * (len(dims) - dim - 1))

    gain = one(*cuts[0])
    for cut in cuts[1:]:
        gain = gain * one(*cut)
    return gain


def centred(rng, shape, width, reach, cuts=(), kind=jnp.bfloat16):
    loudness = shard_levels(rng, shape, cuts, -0.22, 0.18) if cuts else 1.0
    values = jax.random.normal(rng, shape, jnp.float32) * width * loudness
    return jnp.minimum(jnp.maximum(values, -reach), reach).astype(kind)


def setup_inputs(seed: int = 0) -> dict:
    seeds = jax.random.split(jax.random.key(seed), 6)
    fields = centred(seeds[0], (B, H, W, C), 1.0, 6.0, ((0, 8), (1, 64)))
    weight_real = centred(seeds[1], (KX, KY, C, C), C ** -0.5, 0.4375, ((0, 8), (1, 64)))
    weight_imag = centred(seeds[2], (KX, KY, C, C), C ** -0.5, 0.4375, ((0, 8), (1, 64)))
    skip_weight = centred(seeds[3], (C, C), C ** -0.5, 0.4375)
    out_bias = centred(seeds[4], (C,), 0.5, 3.0, (), jnp.float32)
    return {"fields": fields, "weight_real": weight_real, "weight_imag": weight_imag, "skip_weight": skip_weight, "out_bias": out_bias}


def mode_index(number, extent):
    positions = jnp.arange(number, dtype=jnp.int32)
    return jnp.where(positions < number // 2, positions, positions + (extent - number)).astype(jnp.int32)

def phases(left, right, extent):
    product = left[:, None] * right[None, :] % extent
    angles = 2.0 * math.pi / extent * product.astype(jnp.float32)
    return (jnp.cos(angles), jnp.sin(angles))

def column_tables():
    freqs = jnp.arange(KY, dtype=jnp.int32)
    columns = jnp.arange(W, dtype=jnp.int32)
    cos_kw, sin_kw = phases(freqs, columns, W)
    factor = 1.0 / math.sqrt(H * W)
    col_cos = (cos_kw * factor).T
    col_sin = (-sin_kw * factor).T
    doubled = jnp.where(freqs == 0, 1.0, 2.0).astype(jnp.float32) * factor
    back_cos = cos_kw * doubled[:, None]
    back_sin = -sin_kw * doubled[:, None]
    return (col_cos, col_sin, back_cos, back_sin)

def row_tables():
    freqs = mode_index(KX, H)
    rows = jnp.arange(H, dtype=jnp.int32)
    return phases(freqs, rows, H)

def reference(fields, weight_real, weight_imag, skip_weight, out_bias):
    highest = lax.Precision.HIGHEST
    col_cos, col_sin, back_cos, back_sin = column_tables()
    row_cos, row_sin = row_tables()

    def forward_one(field):
        data = field.astype(jnp.float32)
        col_real = jnp.einsum('hwc,wk->hkc', data, col_cos, precision=highest)
        col_imag = jnp.einsum('hwc,wk->hkc', data, col_sin, precision=highest)
        spec_real = jnp.einsum('ih,hkc->ikc', row_cos, col_real, precision=highest) + jnp.einsum('ih,hkc->ikc', row_sin, col_imag, precision=highest)
        spec_imag = jnp.einsum('ih,hkc->ikc', row_cos, col_imag, precision=highest) - jnp.einsum('ih,hkc->ikc', row_sin, col_real, precision=highest)
        return (spec_real.astype(jnp.bfloat16), spec_imag.astype(jnp.bfloat16))
    spec_real, spec_imag = lax.map(forward_one, fields)

    def mix_one(pieces):
        part_real, part_imag, mode_real, mode_imag = pieces
        part_real = part_real.astype(jnp.float32)
        part_imag = part_imag.astype(jnp.float32)
        mode_real = mode_real.astype(jnp.float32)
        mode_imag = mode_imag.astype(jnp.float32)
        out_real = jnp.einsum('bkc,kco->bko', part_real, mode_real, precision=highest) - jnp.einsum('bkc,kco->bko', part_imag, mode_imag, precision=highest)
        out_imag = jnp.einsum('bkc,kco->bko', part_real, mode_imag, precision=highest) + jnp.einsum('bkc,kco->bko', part_imag, mode_real, precision=highest)
        return (out_real, out_imag)
    mix_real, mix_imag = lax.map(mix_one, (spec_real.transpose(1, 0, 2, 3), spec_imag.transpose(1, 0, 2, 3), weight_real, weight_imag))
    mix_real = mix_real.transpose(1, 0, 2, 3)
    mix_imag = mix_imag.transpose(1, 0, 2, 3)

    def inverse_one(pieces):
        field, part_real, part_imag = pieces
        row_real = jnp.einsum('ih,ikc->hkc', row_cos, part_real, precision=highest) - jnp.einsum('ih,ikc->hkc', row_sin, part_imag, precision=highest)
        row_imag = jnp.einsum('ih,ikc->hkc', row_sin, part_real, precision=highest) + jnp.einsum('ih,ikc->hkc', row_cos, part_imag, precision=highest)
        spectral = jnp.einsum('hkc,kw->hwc', row_real, back_cos, precision=highest) + jnp.einsum('hkc,kw->hwc', row_imag, back_sin, precision=highest)
        skip = jnp.dot(field.reshape(-1, C), skip_weight, preferred_element_type=jnp.float32).reshape(spectral.shape)
        return jax.nn.gelu(spectral + skip + out_bias).astype(jnp.bfloat16)
    return lax.map(inverse_one, (fields, mix_real, mix_imag))
```

```python
import functools
import math

import jax
import jax.numpy as jnp
import numpy as np
from jax import lax
from jax.experimental import pallas as pl
from jax.experimental.pallas import tpu as pltpu
from jax.sharding import PartitionSpec as P

MESH = pl.DeviceIdType.MESH
BF = jnp.bfloat16
F32 = jnp.float32
LANES = 128
PAD = 32
GRID = (8, 4, 2)
FAR = (4, 3, 5, 2, 6, 1, 7, 0)


def angles(left, right, extent):
    turn = 2.0 * np.pi / extent * ((left[:, None] * right[None, :]) % extent)
    return np.cos(turn), np.sin(turn)


def packed_tables(H, W, KX, KY, n, nb):
    rows, modes = H // n, KX // nb
    s = 1.0 / math.sqrt(H * W)
    ky = np.arange(KY)
    eye = np.eye(rows)
    cos_w, sin_w = angles(ky, np.arange(W), W)
    g = np.where(ky == 0, 1.0, 2.0)[:, None] * s
    wide = []
    for f in (s, g):
        both = np.stack([cos_w * f, -sin_w * f], 1)
        wide.append(np.einsum("kpw,hg->khpgw", both, eye).reshape(KY * rows * 2, rows * W))
    i = np.arange(KX)
    kx = np.where(i < KX // 2, i, i + H - KX)
    cos_h, sin_h = angles(kx, np.arange(H), H)
    cos_h, sin_h = cos_h.reshape(nb, modes, H), sin_h.reshape(nb, modes, H)
    down = np.zeros((nb, PAD, H, 2))
    down[:, :modes, :, 0], down[:, :modes, :, 1] = cos_h, sin_h
    down[:, modes:2 * modes, :, 0], down[:, modes:2 * modes, :, 1] = -sin_h, cos_h
    up = np.zeros((H, 2, nb, PAD))
    ct, st = cos_h.transpose(2, 0, 1), sin_h.transpose(2, 0, 1)
    up[:, 0, :, :modes], up[:, 0, :, modes:2 * modes] = ct, -st
    up[:, 1, :, :modes], up[:, 1, :, modes:2 * modes] = st, ct
    tables = (wide[0], down.reshape(nb * PAD, 2 * H), up.reshape(2 * H, nb * PAD), wide[1])
    return [jnp.asarray(a.astype(np.float32)).astype(BF) for a in tables]


def dot(a, b, over=(1, 0)):
    return lax.dot_general(a, b, (((over[0],), (over[1],)), ((), ())), preferred_element_type=F32)


def fold(a, tail):
    b0, b1 = a
    return [b0[:LANES], jnp.concatenate([b0[LANES:], b1[LANES:]], axis=0), b1[:LANES]]


def spectral_kernel(
    n, nb, groups, x_ref, wr_ref, wi_ref, skip_ref, bias_ref, first_ref, down_ref, up_ref, last_ref,
    rr_ref, sk_ref, lv_ref,
    xv, fv, dv, uv, wv, sv, csend, crecv, ysend, yrecv, m1, mo, zsend, zrecv, rsend,
    lsem, csem_s, csem_r, ysem_s, ysem_r, zsem_s, zsem_r, rsem_s, rsem_r,
):
    bl, rows, C, W = x_ref.shape
    modes = wr_ref.shape[0]
    tiles = len(groups) and groups[-1][1]
    tail = C - LANES
    used = 2 * modes
    me = lax.axis_index("ma")
    mine = lax.axis_index("ba")
    az, ax, ac = me // 8, (me // 2) % 4, me % 2

    loads = [
        pltpu.make_async_copy(a, b, lsem.at[k]) for k, (a, b) in enumerate((
            (x_ref, xv), (first_ref, fv), (down_ref, dv), (skip_ref, sv),
            (wr_ref.at[:, 0], wv.at[0]), (wi_ref.at[:, 0], wv.at[1]), (up_ref, uv), (last_ref, lv_ref),
        ))
    ]
    for c in loads:
        c.start()

    def peer(dz, r):
        return (az + dz) % 8 * 8 + (ax + r // 2) % 4 * 2 + (ac + r) % 2

    def each_ma(body):
        for dz in FAR:
            @pl.loop(1 if dz == 0 else 0, 8)
            def _(r, dz=dz):
                body(dz * 8 + r, peer(dz, r))

    barrier = pltpu.get_barrier_semaphore()

    @functools.partial(each_ma)
    def _(j, to):
        pl.semaphore_signal(barrier, inc=1, device_id={"ma": to}, device_id_type=MESH)

    @pl.loop(1, nb)
    def _(j):
        pl.semaphore_signal(barrier, inc=1, device_id={"ba": (mine + j) % nb}, device_id_type=MESH)

    zrecv[:, :, used:, :] = jnp.zeros((tiles, nb, PAD - used, LANES), BF)

    def over_ma(src, dst, s, r, q, j, to):
        a, b = groups[q]
        return pltpu.make_async_remote_copy(
            src_ref=src.at[a:b, to], dst_ref=dst.at[a:b, me], send_sem=s.at[q, j],
            recv_sem=r.at[q, j], device_id={"ma": to}, device_id_type=MESH,
        )

    def over_ba(src, dst, s, r, q, j):
        a, b = groups[q]
        to = (mine + j) % nb
        return pltpu.make_async_remote_copy(
            src_ref=src.at[a:b, to, 0:used], dst_ref=dst.at[a:b, mine, 0:used], send_sem=s.at[q, j],
            recv_sem=r.at[q, j], device_id={"ba": to}, device_id_type=MESH,
        )

    def ma_all(what, *refs):
        def go(q):
            each_ma(lambda j, to: getattr(over_ma(*refs, q, j, to), what)())
        return go

    def ba_all(what, *refs):
        def go(q):
            @pl.loop(1, nb)
            def _(j):
                getattr(over_ba(*refs, q, j), what)()
        return go

    cols = (csend, crecv, csem_s, csem_r)
    specs = (ysend, yrecv, ysem_s, ysem_r)
    mixed = (zsend, zrecv, zsem_s, zsem_r)
    lines = (rsend, rr_ref, rsem_s, rsem_r)

    loads[0].wait()
    loads[1].wait()
    x = [
        jnp.concatenate([xv[b, h] for h in range(rows)], axis=1) for b in range(bl)
    ]
    xt = fold(x, tail)
    both = dot(fv[...], jnp.concatenate(xt, axis=0), (1, 1))
    for t in range(tiles):
        csend[t] = both[:, t * LANES:(t + 1) * LANES].astype(BF).reshape(n, 2 * rows, LANES)
    pl.semaphore_wait(barrier, n - 1 + nb - 1)
    for q, (a, b) in enumerate(groups):
        ma_all("start", *cols)(q)
    crecv[:, me] = csend[:, me]

    loads[3].wait()
    turned = sv[...].astype(F32).T.astype(BF)
    wide = jnp.broadcast_to(bias_ref[...], (LANES, C)).T
    bias = jnp.concatenate([wide, wide], axis=1)
    for h in range(rows):
        sk = [dot(turned, xv[b, h]) + bias for b in range(bl)]
        for t, v in enumerate(fold(sk, tail)):
            sk_ref[t, :, h * W:(h + 1) * W] = v

    loads[2].wait()
    for q, (a, b) in enumerate(groups):
        ma_all("wait_recv", *cols)(q)
        col = jnp.concatenate([crecv[t].reshape(n * 2 * rows, LANES) for t in range(a, b)], axis=1)
        spec = dot(dv[...], col).astype(BF)
        for t in range(a, b):
            ysend[t] = spec[:, (t - a) * LANES:(t - a + 1) * LANES].reshape(nb, PAD, LANES)
        ba_all("start", *specs)(q)
        yrecv[a:b, mine] = ysend[a:b, mine]

    for q, (a, b) in enumerate(groups):
        ba_all("wait_recv", *specs)(q)
    for t in range(tiles):
        m1[t] = yrecv[t].reshape(nb * PAD, LANES).astype(F32)
    loads[4].wait()
    loads[5].wait()
    for i in range(modes):
        parts = []
        for p in range(2):
            r = [m1[t, pl.ds(p * modes + i, nb, stride=PAD), :] for t in range(tiles)]
            parts.append([
                jnp.concatenate([r[0], r[1][:, :tail]], axis=1),
                jnp.concatenate([r[2], r[1][:, tail:]], axis=1),
            ])
        re, im = parts
        a1 = jnp.concatenate([re[0], im[0], re[1], im[1]], axis=0).astype(BF)
        a2 = jnp.concatenate([-im[0], re[0], -im[1], re[1]], axis=0).astype(BF)
        o = dot(a1, wv[0, i]) + dot(a2, wv[1, i])
        for p in range(2):
            b0, b1 = o[p * nb:(p + 1) * nb], o[(2 + p) * nb:(3 + p) * nb]
            at = pl.ds(p * modes + i, nb, stride=PAD)
            mo[0, at, :] = b0[:, :LANES]
            mo[1, at, :] = jnp.concatenate([b0[:, LANES:], b1[:, LANES:]], axis=1)
            mo[2, at, :] = b1[:, :LANES]
    for t in range(tiles):
        zsend[t] = mo[t].astype(BF).reshape(nb, PAD, LANES)
    for q, (a, b) in enumerate(groups):
        ba_all("start", *mixed)(q)
    zrecv[:, mine, 0:used] = zsend[:, mine, 0:used]

    loads[6].wait()
    for q, (a, b) in enumerate(groups):
        ba_all("wait_recv", *mixed)(q)
        z = jnp.concatenate([zrecv[t].reshape(nb * PAD, LANES) for t in range(a, b)], axis=1)
        row = dot(uv[...], z).astype(BF)
        for t in range(a, b):
            rsend[t] = row[:, (t - a) * LANES:(t - a + 1) * LANES].reshape(n, 2 * rows, LANES)
        ma_all("start", *lines)(q)
        rr_ref[a:b, me] = rsend[a:b, me]

    loads[7].wait()
    for q in range(len(groups)):
        ma_all("wait_send", *cols)(q)
        ba_all("wait_send", *specs)(q)
        ba_all("wait_send", *mixed)(q)
    for q in range(len(groups)):
        ma_all("wait_recv", *lines)(q)
    for q in range(len(groups)):
        ma_all("wait_send", *lines)(q)


def final_kernel(rr_ref, sk_ref, lv_ref, out_ref, ov, sems):
    bl, rows, C, W = out_ref.shape
    tiles, n = rr_ref.shape[:2]
    tail = C - LANES
    r = jnp.concatenate([rr_ref[t].reshape(-1, LANES) for t in range(tiles)], axis=1)
    rt = r.astype(F32).T.astype(BF)
    copies = []
    for h in range(rows):
        at = slice(h * W, (h + 1) * W)
        spectral = dot(rt, lv_ref[:, at])
        for t in range(tiles):
            v = spectral[t * LANES:(t + 1) * LANES] + sk_ref[t, :, at]
            inner = math.sqrt(2.0 / math.pi) * (v + 0.044715 * (v * v * v))
            o = (0.5 * v * (1.0 + jnp.tanh(inner))).astype(BF)
            if t == 1:
                ov[0, h, LANES:] = o[:tail]
                ov[1, h, LANES:] = o[tail:]
            else:
                ov[t // 2, h, :LANES] = o
        c = pltpu.make_async_copy(ov.at[:, h], out_ref.at[:, h], sems.at[h])
        c.start()
        copies.append(c)
    for c in copies:
        c.wait()


GROUPS = ((0, 3),)


def kernels(n, nb, H, KX, KY, fields, weight_real, weight_imag, skip_weight, out_bias):
    bl, rows, W, C = fields.shape
    modes = weight_real.shape[0]
    first, down, up, last = packed_tables(H, W, KX, KY, n, nb)
    fields = fields.transpose(0, 1, 3, 2)
    vmem = pl.BlockSpec(memory_space=pltpu.VMEM)
    hbm = pl.BlockSpec(memory_space=pl.ANY)
    tiles = bl * C // LANES
    ma_block = pltpu.VMEM((tiles, n, 2 * rows, LANES), BF)
    ba_block = pltpu.VMEM((tiles, nb, PAD, LANES), BF)
    mix_block = pltpu.VMEM((tiles, nb * PAD, LANES), F32)
    dma = pltpu.SemaphoreType.DMA
    ng = len(GROUPS)
    rr, sk, lv = pl.pallas_call(
        functools.partial(spectral_kernel, n, nb, GROUPS),
        out_shape=(
            jax.ShapeDtypeStruct((tiles, n, 2 * rows, LANES), BF),
            jax.ShapeDtypeStruct((tiles, LANES, rows * W), F32),
            jax.ShapeDtypeStruct(last.shape, BF),
        ),
        in_specs=[hbm, hbm, hbm, hbm, vmem, hbm, hbm, hbm, hbm],
        out_specs=(vmem, vmem, vmem),
        scratch_shapes=[
            pltpu.VMEM(fields.shape, BF), pltpu.VMEM(first.shape, BF), pltpu.VMEM(down.shape, BF),
            pltpu.VMEM(up.shape, BF), pltpu.VMEM((2, modes, C, C), BF), pltpu.VMEM((C, C), BF),
            ma_block, ma_block, ba_block, ba_block, mix_block, mix_block, ba_block, ba_block, ma_block,
            dma((8,)), dma((ng, n)), dma((ng, n)), dma((ng, nb)), dma((ng, nb)), dma((ng, nb)),
            dma((ng, nb)), dma((ng, n)), dma((ng, n)),
        ],
        compiler_params=pltpu.CompilerParams(
            collective_id=0, has_side_effects=True, vmem_limit_bytes=48 * 2**20
        ),
        name="spectral",
    )(fields, weight_real, weight_imag, skip_weight, out_bias.reshape(1, C), first, down, up, last)
    out = pl.pallas_call(
        final_kernel,
        out_shape=jax.ShapeDtypeStruct(fields.shape, BF),
        in_specs=[vmem, vmem, vmem],
        out_specs=hbm,
        scratch_shapes=[pltpu.VMEM(fields.shape, BF), dma((rows,))],
        compiler_params=pltpu.CompilerParams(vmem_limit_bytes=16 * 2**20),
        name="finish",
    )(rr, sk, lv)
    return out.transpose(0, 1, 3, 2)


def solution(mesh):
    n, nb = mesh.shape["ma"], mesh.shape["ba"]

    def local(fields, weight_real, weight_imag, skip_weight, out_bias):
        sizes = (fields.shape[1] * n, weight_real.shape[0] * nb, weight_real.shape[1] * n)
        return kernels(n, nb, *sizes, fields, weight_real, weight_imag, skip_weight, out_bias)

    split = P("ba", "ma", None, None)
    return jax.shard_map(
        local, mesh=mesh, in_specs=(split, split, split, P(), P()), out_specs=split, check_vma=False
    )
```

```python
import functools
import math

import jax
import jax.numpy as jnp
import numpy as np
from jax import lax
from jax.experimental import pallas as pl
from jax.experimental.pallas import tpu as pltpu
from jax.sharding import PartitionSpec as P

MESH = pl.DeviceIdType.MESH
BF = jnp.bfloat16
F32 = jnp.float32
LANES = 128
PAD = 32
GRID = (8, 4, 2)
FAR = (4, 3, 5, 2, 6, 1, 7, 0)


def angles(left, right, extent):
    turn = 2.0 * np.pi / extent * ((left[:, None] * right[None, :]) % extent)
    return np.cos(turn), np.sin(turn)


def packed_tables(H, W, KX, KY, n, nb):
    rows, modes = H // n, KX // nb
    s = 1.0 / math.sqrt(H * W)
    ky = np.arange(KY)
    eye = np.eye(rows)
    cos_w, sin_w = angles(ky, np.arange(W), W)
    g = np.where(ky == 0, 1.0, 2.0)[:, None] * s
    wide = []
    for f in (s, g):
        both = np.stack([cos_w * f, -sin_w * f], 1)
        wide.append(np.einsum("kpw,hg->khpgw", both, eye).reshape(KY * rows * 2, rows * W))
    i = np.arange(KX)
    kx = np.where(i < KX // 2, i, i + H - KX)
    cos_h, sin_h = angles(kx, np.arange(H), H)
    cos_h, sin_h = cos_h.reshape(nb, modes, H), sin_h.reshape(nb, modes, H)
    down = np.zeros((nb, PAD, H, 2))
    down[:, :modes, :, 0], down[:, :modes, :, 1] = cos_h, sin_h
    down[:, modes:2 * modes, :, 0], down[:, modes:2 * modes, :, 1] = -sin_h, cos_h
    up = np.zeros((H, 2, nb, PAD))
    ct, st = cos_h.transpose(2, 0, 1), sin_h.transpose(2, 0, 1)
    up[:, 0, :, :modes], up[:, 0, :, modes:2 * modes] = ct, -st
    up[:, 1, :, :modes], up[:, 1, :, modes:2 * modes] = st, ct
    tables = (wide[0], down.reshape(nb * PAD, 2 * H), up.reshape(2 * H, nb * PAD), wide[1])
    return [jnp.asarray(a.astype(np.float32)).astype(BF) for a in tables]


def dot(a, b, over=(1, 0)):
    return lax.dot_general(a, b, (((over[0],), (over[1],)), ((), ())), preferred_element_type=F32)


def fold(a, tail):
    b0, b1 = a
    return [b0[:LANES], jnp.concatenate([b0[LANES:], b1[LANES:]], axis=0), b1[:LANES]]


def spectral_kernel(
    n, nb, groups, x_ref, wr_ref, wi_ref, skip_ref, bias_ref, first_ref, down_ref, up_ref, last_ref,
    rr_ref, sk_ref, lv_ref,
    xv, fv, dv, uv, wv, sv, bv, csend, crecv, ysend, yrecv, m1, mo, zsend, zrecv, rsend,
    lsem, csem_s, csem_r, ysem_s, ysem_r, zsem_s, zsem_r, rsem_s, rsem_r,
):
    bl, rows, C, W = x_ref.shape
    modes = wr_ref.shape[0]
    tiles = len(groups) and groups[-1][1]
    tail = C - LANES
    used = 2 * modes
    me = lax.axis_index("ma")
    mine = lax.axis_index("ba")
    az, ax, ac = me // 8, (me // 2) % 4, me % 2

    loads = [
        pltpu.make_async_copy(a, b, lsem.at[k]) for k, (a, b) in enumerate((
            (x_ref, xv), (first_ref, fv), (down_ref, dv), (skip_ref, sv),
            (wr_ref.at[:, 0], wv.at[0]), (wi_ref.at[:, 0], wv.at[1]), (up_ref, uv), (last_ref, lv_ref),
            (bias_ref, bv),
        ))
    ]
    for c in loads:
        c.start()

    def peer(dz, r):
        return (az + dz) % 8 * 8 + (ax + r // 2) % 4 * 2 + (ac + r) % 2

    def each_ma(body):
        @pl.loop(0, 8)
        def _(r):
            for dz in FAR[:-1]:
                body(dz * 8 + r, peer(dz, r))

        @pl.loop(1, 8)
        def _(r):
            body(r, peer(0, r))

    barrier = pltpu.get_barrier_semaphore()

    @functools.partial(each_ma)
    def _(j, to):
        pl.semaphore_signal(barrier, inc=1, device_id={"ma": to}, device_id_type=MESH)

    @pl.loop(1, nb)
    def _(j):
        pl.semaphore_signal(barrier, inc=1, device_id={"ba": (mine + j) % nb}, device_id_type=MESH)

    zrecv[:, :, used:, :] = jnp.zeros((tiles, nb, PAD - used, LANES), BF)

    def over_ma(src, dst, s, r, q, j, to):
        a, b = groups[q]
        return pltpu.make_async_remote_copy(
            src_ref=src.at[a:b, to], dst_ref=dst.at[a:b, me], send_sem=s.at[q, j],
            recv_sem=r.at[q, j], device_id={"ma": to}, device_id_type=MESH,
        )

    def over_ba(src, dst, s, r, q, j):
        a, b = groups[q]
        to = (mine + j) % nb
        return pltpu.make_async_remote_copy(
            src_ref=src.at[a:b, to, 0:used], dst_ref=dst.at[a:b, mine, 0:used], send_sem=s.at[q, j],
            recv_sem=r.at[q, j], device_id={"ba": to}, device_id_type=MESH,
        )

    def ma_all(what, *refs):
        def go(q):
            each_ma(lambda j, to: getattr(over_ma(*refs, q, j, to), what)())
        return go

    def ba_all(what, *refs):
        def go(q):
            @pl.loop(1, nb)
            def _(j):
                getattr(over_ba(*refs, q, j), what)()
        return go

    cols = (csend, crecv, csem_s, csem_r)
    specs = (ysend, yrecv, ysem_s, ysem_r)
    mixed = (zsend, zrecv, zsem_s, zsem_r)
    lines = (rsend, rr_ref, rsem_s, rsem_r)

    loads[0].wait()
    loads[1].wait()
    x = [
        jnp.concatenate([xv[b, h] for h in range(rows)], axis=1) for b in range(bl)
    ]
    xt = fold(x, tail)
    both = dot(fv[...], jnp.concatenate(xt, axis=0), (1, 1))
    for t in range(tiles):
        csend[t] = both[:, t * LANES:(t + 1) * LANES].astype(BF).reshape(n, 2 * rows, LANES)
    pl.semaphore_wait(barrier, n - 1 + nb - 1)
    for q, (a, b) in enumerate(groups):
        ma_all("start", *cols)(q)
    crecv[:, me] = csend[:, me]

    loads[3].wait()
    loads[8].wait()
    turned = sv[...].astype(F32).T.astype(BF)
    wide = jnp.broadcast_to(bv[...], (LANES, C)).T
    bias = jnp.concatenate([wide, wide], axis=1)
    for h in range(rows):
        sk = [dot(turned, xv[b, h]) + bias for b in range(bl)]
        for t, v in enumerate(fold(sk, tail)):
            sk_ref[t, :, h * W:(h + 1) * W] = v

    loads[2].wait()
    for q, (a, b) in enumerate(groups):
        ma_all("wait_recv", *cols)(q)
        col = jnp.concatenate([crecv[t].reshape(n * 2 * rows, LANES) for t in range(a, b)], axis=1)
        spec = dot(dv[...], col).astype(BF)
        for t in range(a, b):
            ysend[t] = spec[:, (t - a) * LANES:(t - a + 1) * LANES].reshape(nb, PAD, LANES)
        ba_all("start", *specs)(q)
        yrecv[a:b, mine] = ysend[a:b, mine]

    for q, (a, b) in enumerate(groups):
        ba_all("wait_recv", *specs)(q)
    for t in range(tiles):
        m1[t] = yrecv[t].reshape(nb * PAD, LANES).astype(F32)
    loads[4].wait()
    loads[5].wait()
    for i in range(modes):
        parts = []
        for p in range(2):
            r = [m1[t, pl.ds(p * modes + i, nb, stride=PAD), :] for t in range(tiles)]
            parts.append([
                jnp.concatenate([r[0], r[1][:, :tail]], axis=1),
                jnp.concatenate([r[2], r[1][:, tail:]], axis=1),
            ])
        re, im = parts
        a1 = jnp.concatenate([re[0], im[0], re[1], im[1]], axis=0).astype(BF)
        a2 = jnp.concatenate([-im[0], re[0], -im[1], re[1]], axis=0).astype(BF)
        o = dot(a1, wv[0, i]) + dot(a2, wv[1, i])
        for p in range(2):
            b0, b1 = o[p * nb:(p + 1) * nb], o[(2 + p) * nb:(3 + p) * nb]
            at = pl.ds(p * modes + i, nb, stride=PAD)
            mo[0, at, :] = b0[:, :LANES]
            mo[1, at, :] = jnp.concatenate([b0[:, LANES:], b1[:, LANES:]], axis=1)
            mo[2, at, :] = b1[:, :LANES]
    for t in range(tiles):
        zsend[t] = mo[t].astype(BF).reshape(nb, PAD, LANES)
    for q, (a, b) in enumerate(groups):
        ba_all("start", *mixed)(q)
    zrecv[:, mine, 0:used] = zsend[:, mine, 0:used]

    loads[6].wait()
    for q, (a, b) in enumerate(groups):
        ba_all("wait_recv", *mixed)(q)
        z = jnp.concatenate([zrecv[t].reshape(nb * PAD, LANES) for t in range(a, b)], axis=1)
        row = dot(uv[...], z).astype(BF)
        for t in range(a, b):
            rsend[t] = row[:, (t - a) * LANES:(t - a + 1) * LANES].reshape(n, 2 * rows, LANES)
        ma_all("start", *lines)(q)
        rr_ref[a:b, me] = rsend[a:b, me]

    loads[7].wait()
    for q in range(len(groups)):
        ma_all("wait_send", *cols)(q)
        ba_all("wait_send", *specs)(q)
        ba_all("wait_send", *mixed)(q)
    for q in range(len(groups)):
        ma_all("wait_recv", *lines)(q)
    for q in range(len(groups)):
        ma_all("wait_send", *lines)(q)


def final_kernel(rr_ref, sk_ref, lv_ref, out_ref, ov, sems):
    bl, rows, C, W = out_ref.shape
    tiles, n = rr_ref.shape[:2]
    tail = C - LANES
    r = jnp.concatenate([rr_ref[t].reshape(-1, LANES) for t in range(tiles)], axis=1)
    rt = r.astype(F32).T.astype(BF)
    copies = []
    for h in range(rows):
        at = slice(h * W, (h + 1) * W)
        spectral = dot(rt, lv_ref[:, at])
        for t in range(tiles):
            v = spectral[t * LANES:(t + 1) * LANES] + sk_ref[t, :, at]
            inner = math.sqrt(2.0 / math.pi) * (v + 0.044715 * (v * v * v))
            o = (0.5 * v * (1.0 + jnp.tanh(inner))).astype(BF)
            if t == 1:
                ov[0, h, LANES:] = o[:tail]
                ov[1, h, LANES:] = o[tail:]
            else:
                ov[t // 2, h, :LANES] = o
        c = pltpu.make_async_copy(ov.at[:, h], out_ref.at[:, h], sems.at[h])
        c.start()
        copies.append(c)
    for c in copies:
        c.wait()


GROUPS = ((0, 3),)


def kernels(n, nb, H, KX, KY, fields, weight_real, weight_imag, skip_weight, out_bias):
    bl, rows, W, C = fields.shape
    modes = weight_real.shape[0]
    first, down, up, last = packed_tables(H, W, KX, KY, n, nb)
    fields = fields.transpose(0, 1, 3, 2)
    vmem = pl.BlockSpec(memory_space=pltpu.VMEM)
    hbm = pl.BlockSpec(memory_space=pltpu.HBM)
    tiles = bl * C // LANES
    ma_block = pltpu.VMEM((tiles, n, 2 * rows, LANES), BF)
    ba_block = pltpu.VMEM((tiles, nb, PAD, LANES), BF)
    mix_block = pltpu.VMEM((tiles, nb * PAD, LANES), F32)
    dma = pltpu.SemaphoreType.DMA
    ng = len(GROUPS)
    rr, sk, lv = pl.pallas_call(
        functools.partial(spectral_kernel, n, nb, GROUPS),
        out_shape=(
            jax.ShapeDtypeStruct((tiles, n, 2 * rows, LANES), BF),
            jax.ShapeDtypeStruct((tiles, LANES, rows * W), F32),
            jax.ShapeDtypeStruct(last.shape, BF),
        ),
        in_specs=[hbm] * 9,
        out_specs=(vmem, vmem, vmem),
        scratch_shapes=[
            pltpu.VMEM(fields.shape, BF), pltpu.VMEM(first.shape, BF), pltpu.VMEM(down.shape, BF),
            pltpu.VMEM(up.shape, BF), pltpu.VMEM((2, modes, C, C), BF), pltpu.VMEM((C, C), BF), pltpu.VMEM((1, C), F32),
            ma_block, ma_block, ba_block, ba_block, mix_block, mix_block, ba_block, ba_block, ma_block,
            dma((9,)), dma((ng, n)), dma((ng, n)), dma((ng, nb)), dma((ng, nb)), dma((ng, nb)),
            dma((ng, nb)), dma((ng, n)), dma((ng, n)),
        ],
        compiler_params=pltpu.CompilerParams(
            collective_id=0, has_side_effects=True, vmem_limit_bytes=20 * 2**20
        ),
        name="spectral",
    )(*[
        pltpu.with_memory_space_constraint(a, pltpu.HBM)
        for a in (fields, weight_real, weight_imag, skip_weight, out_bias.reshape(1, C), first, down, up, last)
    ])
    out = pl.pallas_call(
        final_kernel,
        out_shape=jax.ShapeDtypeStruct(fields.shape, BF),
        in_specs=[vmem, vmem, vmem],
        out_specs=hbm,
        scratch_shapes=[pltpu.VMEM(fields.shape, BF), dma((rows,))],
        compiler_params=pltpu.CompilerParams(vmem_limit_bytes=16 * 2**20),
        name="finish",
    )(rr, sk, lv)
    return out.transpose(0, 1, 3, 2)


def solution(mesh):
    n, nb = mesh.shape["ma"], mesh.shape["ba"]

    def local(fields, weight_real, weight_imag, skip_weight, out_bias):
        sizes = (fields.shape[1] * n, weight_real.shape[0] * nb, weight_real.shape[1] * n)
        return kernels(n, nb, *sizes, fields, weight_real, weight_imag, skip_weight, out_bias)

    split = P("ba", "ma", None, None)
    return jax.shard_map(
        local, mesh=mesh, in_specs=(split, split, split, P(), P()), out_specs=split, check_vma=False
    )
```

```python
import functools
import math

import jax
import jax.numpy as jnp
import numpy as np
from jax import lax
from jax.experimental import pallas as pl
from jax.experimental.pallas import tpu as pltpu
from jax.sharding import PartitionSpec as P

MESH = pl.DeviceIdType.MESH
BF = jnp.bfloat16
F32 = jnp.float32
LANES = 128
HALF = 64
PAD = 16
FAR = (4, 3, 5, 2, 6, 1, 7)


def angles(left, right, extent):
    turn = 2.0 * np.pi / extent * ((left[:, None] * right[None, :]) % extent)
    return np.cos(turn), np.sin(turn)


def packed_tables(H, W, KX, KY, n, nb):
    rows, modes = H // n, KX // nb
    s = 1.0 / math.sqrt(H * W)
    ky = np.arange(KY)
    eye = np.eye(rows)
    cos_w, sin_w = angles(ky, np.arange(W), W)
    g = np.where(ky == 0, 1.0, 2.0)[:, None] * s
    wide = []
    for f in (s, g):
        both = np.stack([cos_w * f, -sin_w * f], 0)
        wide.append(np.einsum("pkw,hg->pkhgw", both, eye).reshape(2 * KY * rows, rows * W))
    i = np.arange(KX)
    kx = np.where(i < KX // 2, i, i + H - KX)
    both = np.stack(angles(kx, np.arange(H), H), 0).reshape(2, nb, modes, H)
    both = np.pad(both, ((0, 0), (0, 0), (0, PAD - modes), (0, 0))).reshape(2, nb * PAD, H)
    down = both.reshape(2 * nb * PAD, H)
    up = both.transpose(0, 2, 1).reshape(2 * H, nb * PAD)
    return [jnp.asarray(a.astype(np.float32)).astype(BF) for a in (wide[0], down, up, wide[1])]


def dot(a, b, over=(1, 0)):
    return lax.dot_general(a, b, (((over[0],), (over[1],)), ((), ())), preferred_element_type=F32)


def lane(a, k):
    return a[:, k * HALF:(k + 1) * HALF]


def side(a, b):
    return jnp.concatenate([a, b], axis=1)


def turn(both, sign):
    m = both.shape[0] // 2
    low = lax.broadcasted_iota(jnp.int32, (m, LANES), 1) < HALF
    out = []
    for k in range(both.shape[1] // LANES):
        p, q = both[:m, k * LANES:(k + 1) * LANES], both[m:, k * LANES:(k + 1) * LANES]
        q = side(lane(q, 1), lane(q, 0))
        out.append(p + jnp.where(low, sign * q, -sign * q))
    return out


def last_step(parts, lv_ref, at, sk):
    rt = []
    for r in parts:
        t = r.astype(F32).T.astype(BF)
        rt.append(side(t[:HALF], t[HALF:]))
    v = dot(jnp.concatenate(rt, axis=0), lv_ref[:, at]) + sk
    inner = math.sqrt(2.0 / math.pi) * (v + 0.044715 * (v * v * v))
    return (0.5 * v * (1.0 + jnp.tanh(inner))).astype(BF)


def spectral_kernel(
    n, nb, x_ref, wr_ref, wi_ref, skip_ref, bias_ref, first_ref, down_ref, up_ref, last_ref,
    done_ref, rr_ref, sk_ref, lv_ref,
    xv, fv, dv, uv, wv, sv, bv, csend, crecv, ysend, yrecv, m1, mo, zsend, zrecv, rsend, rr0, sk0,
    lsem, send_sem, recv_sem,
):
    bl, rows, C, W = x_ref.shape
    modes = wr_ref.shape[0]
    parts = C // HALF
    me = lax.axis_index("ma")
    mine = lax.axis_index("ba")
    az, ax, ac = me // 8, (me // 2) % 4, me % 2

    loads = [
        pltpu.make_async_copy(a, b, lsem.at[k]) for k, (a, b) in enumerate((
            (x_ref, xv), (first_ref, fv), (down_ref, dv), (skip_ref, sv),
            (wr_ref.at[:, 0], wv.at[0]), (wi_ref.at[:, 0], wv.at[1]), (up_ref, uv), (last_ref, lv_ref),
            (bias_ref, bv),
        ))
    ]
    for c in loads:
        c.start()

    def peer(dz, r):
        return (az + dz) % 8 * 8 + (ax + r // 2) % 4 * 2 + (ac + r) % 2

    def each_ma(body):
        @pl.loop(0, 8)
        def _(r):
            for dz in FAR:
                body(peer(dz, r))

        @pl.loop(1, 8)
        def _(r):
            body(peer(0, r))

    def each_ba(body):
        for j in (4, 3, 5, 2, 6, 1, 7):
            body((mine + j) % nb)

    barrier = pltpu.get_barrier_semaphore()
    each_ma(lambda to: pl.semaphore_signal(barrier, inc=1, device_id={"ma": to}, device_id_type=MESH))
    each_ba(lambda to: pl.semaphore_signal(barrier, inc=1, device_id={"ba": to}, device_id_type=MESH))

    zrecv[:, :, modes:, :] = jnp.zeros((bl * parts, nb, PAD - modes, LANES), BF)

    def group(ref, b):
        return ref if ref.shape[0] == parts else ref.at[parts * b:parts * (b + 1)]

    class Exchange:
        def __init__(self, kind, axis, each, here, count, send, recv, used=None):
            self.kind, self.axis, self.each, self.here, self.count = kind, axis, each, here, count
            self.send, self.recv, self.used = send, recv, used

        def block(self, ref, b, d):
            v = group(ref, b)
            return v.at[:, d] if self.used is None else v.at[:, d, 0:self.used]

        def start(self, b):
            def go(to):
                pltpu.make_async_remote_copy(
                    src_ref=self.block(self.send, b, to), dst_ref=self.block(self.recv[b], b, self.here),
                    send_sem=send_sem.at[self.kind, b], recv_sem=recv_sem.at[self.kind, b],
                    device_id={self.axis: to}, device_id_type=MESH,
                ).start()

            self.each(go)
            self.block(self.recv[b], b, self.here)[...] = self.block(self.send, b, self.here)[...]

        def wait(self, ref, b, sem):
            every = self.block(ref, b, slice(0, self.count))
            pltpu.make_async_copy(every, every, sem.at[self.kind, b]).wait()

        def wait_recv(self, b):
            self.wait(self.recv[b], b, recv_sem)

        def wait_send(self, b):
            self.wait(self.send, b, send_sem)

    cols = Exchange(0, "ma", each_ma, me, n - 1, csend, (crecv, crecv))
    specs = Exchange(1, "ba", each_ba, mine, nb - 1, ysend, (yrecv, yrecv), modes)
    mixed = Exchange(2, "ba", each_ba, mine, nb - 1, zsend, (zrecv, zrecv), modes)
    lines = Exchange(3, "ma", each_ma, me, n - 1, rsend, (rr0, rr_ref))

    loads[0].wait()
    loads[1].wait()
    for b in range(bl):
        both = dot(fv[...], jnp.concatenate([xv[b, h] for h in range(rows)], axis=1), (1, 1))
        re, im = both[:n * rows], both[n * rows:]
        for k in range(parts):
            csend[b * parts + k] = side(lane(re, k), lane(im, k)).astype(BF).reshape(n, rows, LANES)
        if b == 0:
            pl.semaphore_wait(barrier, n - 1 + nb - 1)
        cols.start(b)

    loads[3].wait()
    loads[8].wait()
    turned = sv[...].astype(F32).T.astype(BF)
    wide = jnp.broadcast_to(bv[...], (LANES, C)).T
    bias = jnp.concatenate([wide, wide], axis=1)
    for b in range(bl):
        for h in range(rows):
            (sk0, sk_ref)[b][:, h * W:(h + 1) * W] = dot(turned, xv[b, h]) + bias

    def rows_down(b):
        cols.wait_recv(b)
        col = jnp.concatenate([crecv[b * parts + k].reshape(n * rows, LANES) for k in range(parts)], axis=1)
        for k, v in enumerate(turn(dot(dv[...], col), 1.0)):
            ysend[b * parts + k] = v.astype(BF).reshape(nb, PAD, LANES)
        specs.start(b)

    def mix(b):
        specs.wait_recv(b)
        for k in range(parts):
            m1[k] = yrecv[b * parts + k].reshape(nb * PAD, LANES).astype(F32)
        for i in range(modes):
            at = pl.ds(i, nb, stride=PAD)
            v = [m1[k, at, :] for k in range(parts)]
            re, im = [jnp.concatenate([lane(a, p) for a in v], axis=1) for p in range(2)]
            a1 = jnp.concatenate([re, im], axis=0).astype(BF)
            a2 = jnp.concatenate([-im, re], axis=0).astype(BF)
            o = dot(a1, wv[0, i]) + dot(a2, wv[1, i])
            for k in range(parts):
                mo[k, at, :] = side(lane(o[:nb], k), lane(o[nb:], k))
        for k in range(parts):
            zsend[b * parts + k] = mo[k].astype(BF).reshape(nb, PAD, LANES)
        mixed.start(b)

    def rows_up(b):
        mixed.wait_recv(b)
        z = jnp.concatenate([zrecv[b * parts + k].reshape(nb * PAD, LANES) for k in range(parts)], axis=1)
        for k, v in enumerate(turn(dot(uv[...], z), -1.0)):
            rsend[b * parts + k] = v.astype(BF).reshape(n, rows, LANES)
        lines.start(b)

    loads[2].wait()
    rows_down(0)
    rows_down(1)
    loads[4].wait()
    loads[5].wait()
    mix(0)
    mix(1)
    loads[6].wait()
    rows_up(0)
    rows_up(1)
    loads[7].wait()
    for e in (cols, specs, mixed):
        for b in range(bl):
            e.wait_send(b)
    lines.wait_recv(0)
    for h in range(rows):
        at = slice(h * W, (h + 1) * W)
        done_ref[h] = last_step([rr0[k].reshape(n * rows, LANES) for k in range(parts)], lv_ref, at, sk0[:, at])
    lines.wait_recv(1)
    for b in range(bl):
        lines.wait_send(b)


def final_kernel(done_ref, rr_ref, sk_ref, lv_ref, out_ref, ov, sems):
    bl, rows, C, W = out_ref.shape
    parts = C // HALF
    copies = [pltpu.make_async_copy(done_ref, out_ref.at[0], sems.at[rows])]
    copies[0].start()
    r = [rr_ref[k].reshape(-1, LANES) for k in range(parts)]
    for h in range(rows):
        at = slice(h * W, (h + 1) * W)
        ov[h] = last_step(r, lv_ref, at, sk_ref[:, at])
        c = pltpu.make_async_copy(ov.at[h], out_ref.at[1, h], sems.at[h])
        c.start()
        copies.append(c)
    for c in copies:
        c.wait()


def kernels(n, nb, H, KX, KY, fields, weight_real, weight_imag, skip_weight, out_bias):
    bl, rows, W, C = fields.shape
    modes = weight_real.shape[0]
    first, down, up, last = packed_tables(H, W, KX, KY, n, nb)
    fields = fields.transpose(0, 1, 3, 2)
    vmem = pl.BlockSpec(memory_space=pltpu.VMEM)
    hbm = pl.BlockSpec(memory_space=pltpu.HBM)
    parts = C // HALF
    half_block = (parts, n, rows, LANES)
    skip_block = (C, rows * W)
    ma_block = pltpu.VMEM((bl * parts, n, rows, LANES), BF)
    ba_block = pltpu.VMEM((bl * parts, nb, PAD, LANES), BF)
    mix_block = pltpu.VMEM((parts, nb * PAD, LANES), F32)
    dma = pltpu.SemaphoreType.DMA
    half = pl.pallas_call(
        functools.partial(spectral_kernel, n, nb),
        out_shape=(
            jax.ShapeDtypeStruct(fields.shape[1:], BF),
            jax.ShapeDtypeStruct(half_block, BF),
            jax.ShapeDtypeStruct(skip_block, F32),
            jax.ShapeDtypeStruct(last.shape, BF),
        ),
        in_specs=[hbm] * 9,
        out_specs=(vmem,) * 4,
        scratch_shapes=[
            pltpu.VMEM(fields.shape, BF), pltpu.VMEM(first.shape, BF), pltpu.VMEM(down.shape, BF),
            pltpu.VMEM(up.shape, BF), pltpu.VMEM((2, modes, C, C), BF), pltpu.VMEM((C, C), BF),
            pltpu.VMEM((1, C), F32), ma_block, ma_block, ba_block, ba_block, mix_block, mix_block,
            ba_block, ba_block, ma_block, pltpu.VMEM(half_block, BF), pltpu.VMEM(skip_block, F32),
            dma((9,)), dma((4, bl)), dma((4, bl)),
        ],
        compiler_params=pltpu.CompilerParams(
            collective_id=0, has_side_effects=True, vmem_limit_bytes=24 * 2**20
        ),
        name="spectral",
    )(*[
        pltpu.with_memory_space_constraint(a, pltpu.HBM)
        for a in (fields, weight_real, weight_imag, skip_weight, out_bias.reshape(1, C), first, down, up, last)
    ])
    out = pl.pallas_call(
        final_kernel,
        out_shape=jax.ShapeDtypeStruct(fields.shape, BF),
        in_specs=[vmem] * 4,
        out_specs=hbm,
        scratch_shapes=[pltpu.VMEM(fields.shape[1:], BF), dma((rows + 1,))],
        compiler_params=pltpu.CompilerParams(vmem_limit_bytes=16 * 2**20),
        name="finish",
    )(*half)
    return out.transpose(0, 1, 3, 2)


def solution(mesh):
    n, nb = mesh.shape["ma"], mesh.shape["ba"]

    def local(fields, weight_real, weight_imag, skip_weight, out_bias):
        sizes = (fields.shape[1] * n, weight_real.shape[0] * nb, weight_real.shape[1] * n)
        return kernels(n, nb, *sizes, fields, weight_real, weight_imag, skip_weight, out_bias)

    split = P("ba", "ma", None, None)
    return jax.shard_map(
        local, mesh=mesh, in_specs=(split, split, split, P(), P()), out_specs=split, check_vma=False
    )
```

```python
import functools
import math

import jax
import jax.numpy as jnp
import numpy as np
from jax import lax
from jax.experimental import pallas as pl
from jax.experimental.pallas import tpu as pltpu
from jax.sharding import PartitionSpec as P

MESH = pl.DeviceIdType.MESH
BF = jnp.bfloat16
F32 = jnp.float32
LANES = 128
HALF = 64
PAD = 16
TURNS = (4, 5, 3, 6, 2, 7, 1)


def offsets():
    out = [
        (dz, dx, dc) for dc in (1, 0) for dxs in ((2,), (1, 3), (0,)) for dz in TURNS for dx in dxs
    ]
    return out + [(0, dx, dc) for dx, dc in ((2, 1), (2, 0), (1, 1), (3, 1), (1, 0), (3, 0), (0, 1))]


def hops(o):
    return min(o[0], 8 - o[0]) + min(o[1], 4 - o[1])


def angles(left, right, extent):
    turn = 2.0 * np.pi / extent * ((left[:, None] * right[None, :]) % extent)
    return np.cos(turn), np.sin(turn)


def packed_tables(H, W, KX, KY, n, nb):
    rows, modes = H // n, KX // nb
    s = 1.0 / math.sqrt(H * W)
    ky = np.arange(KY)
    eye = np.eye(rows)
    cos_w, sin_w = angles(ky, np.arange(W), W)
    g = np.where(ky == 0, 1.0, 2.0)[:, None] * s
    wide = []
    for f in (s, g):
        both = np.stack([cos_w * f, -sin_w * f], 0)
        wide.append(np.einsum("pkw,hg->pkhgw", both, eye).reshape(2 * KY * rows, rows * W))
    i = np.arange(KX)
    kx = np.where(i < KX // 2, i, i + H - KX)
    both = np.stack(angles(kx, np.arange(H), H), 0).reshape(2, nb, modes, H)
    both = np.pad(both, ((0, 0), (0, 0), (0, PAD - modes), (0, 0))).reshape(2, nb * PAD, H)
    down = both.reshape(2 * nb * PAD, H)
    up = both.transpose(0, 2, 1).reshape(2 * H, nb * PAD)
    return [jnp.asarray(a.astype(np.float32)).astype(BF) for a in (wide[0], down, up, wide[1])]


def dot(a, b, over=(1, 0)):
    return lax.dot_general(a, b, (((over[0],), (over[1],)), ((), ())), preferred_element_type=F32)


def lane(a, k):
    return a[:, k * HALF:(k + 1) * HALF]


def side(a, b):
    return jnp.concatenate([a, b], axis=1)


def turn(both, sign):
    m = both.shape[0] // 2
    low = lax.broadcasted_iota(jnp.int32, (m, LANES), 1) < HALF
    out = []
    for k in range(both.shape[1] // LANES):
        p, q = both[:m, k * LANES:(k + 1) * LANES], both[m:, k * LANES:(k + 1) * LANES]
        q = side(lane(q, 1), lane(q, 0))
        out.append(p + jnp.where(low, sign * q, -sign * q))
    return out


def turned_lines(parts):
    out = []
    for r in parts:
        t = r.astype(F32).T.astype(BF)
        out.append(side(t[:HALF], t[HALF:]))
    return jnp.concatenate(out, axis=0)


def last_step(rt, lv_ref, at, sk):
    v = dot(rt, lv_ref[:, at]) + sk
    c = math.sqrt(2.0 / math.pi)
    half = 0.5 * v
    return (half + half * jnp.tanh(v * (c + (0.044715 * c) * (v * v)))).astype(BF)


def spectral_kernel(
    n, nb, x_ref, wr_ref, wi_ref, skip_ref, bias_ref, first_ref, down_ref, up_ref, last_ref,
    done_ref, rr_ref, sk_ref, lv_ref,
    xv, fv, dv, uv, wv, sv, bv, csend, crecv, ysend, yrecv, m1, mo, zsend, zrecv, rsend, rr0, sk0,
    lsem, send_sem, recv_sem,
):
    bl, rows, C, W = x_ref.shape
    modes = wr_ref.shape[0]
    parts = C // HALF
    me = lax.axis_index("ma")
    mine = lax.axis_index("ba")
    az, ax, ac = me // 8, (me // 2) % 4, me % 2

    loads = [
        pltpu.make_async_copy(a, b, lsem.at[k]) for k, (a, b) in enumerate((
            (x_ref, xv), (first_ref, fv), (down_ref, dv), (skip_ref, sv),
            (wr_ref.at[:, 0], wv.at[0]), (wi_ref.at[:, 0], wv.at[1]), (up_ref, uv), (last_ref, lv_ref),
            (bias_ref, bv),
        ))
    ]
    for c in loads:
        c.start()

    def peer(dz, dx, dc):
        return (az + dz) % 8 * 8 + (ax + dx) % 4 * 2 + (ac + dc) % 2

    def each_ma(body):
        for o in offsets():
            body(peer(*o))

    def each_ba(body):
        for j in (4, 3, 5, 2, 6, 1, 7):
            body((mine + j) % nb)

    barrier = pltpu.get_barrier_semaphore()
    for o in sorted(offsets(), key=lambda o: -hops(o)):
        pl.semaphore_signal(barrier, inc=1, device_id={"ma": peer(*o)}, device_id_type=MESH)
    each_ba(lambda to: pl.semaphore_signal(barrier, inc=1, device_id={"ba": to}, device_id_type=MESH))

    zrecv[:, :, modes:, :] = jnp.zeros((bl * parts, nb, PAD - modes, LANES), BF)

    def group(ref, b):
        return ref if ref.shape[0] == parts else ref.at[parts * b:parts * (b + 1)]

    class Exchange:
        def __init__(self, kind, axis, each, here, count, send, recv, used=None):
            self.kind, self.axis, self.each, self.here, self.count = kind, axis, each, here, count
            self.send, self.recv, self.used = send, recv, used

        def block(self, ref, b, d):
            v = group(ref, b)
            return v.at[:, d] if self.used is None else v.at[:, d, 0:self.used]

        def start(self, b):
            def go(to):
                pltpu.make_async_remote_copy(
                    src_ref=self.block(self.send, b, to), dst_ref=self.block(self.recv[b], b, self.here),
                    send_sem=send_sem.at[self.kind, b], recv_sem=recv_sem.at[self.kind, b],
                    device_id={self.axis: to}, device_id_type=MESH,
                ).start()

            self.each(go)
            self.block(self.recv[b], b, self.here)[...] = self.block(self.send, b, self.here)[...]

        def wait(self, ref, b, sem):
            every = self.block(ref, b, slice(0, self.count))
            pltpu.make_async_copy(every, every, sem.at[self.kind, b]).wait()

        def wait_recv(self, b):
            self.wait(self.recv[b], b, recv_sem)

        def wait_send(self, b):
            self.wait(self.send, b, send_sem)

    cols = Exchange(0, "ma", each_ma, me, n - 1, csend, (crecv, crecv))
    specs = Exchange(1, "ba", each_ba, mine, nb - 1, ysend, (yrecv, yrecv), modes)
    mixed = Exchange(2, "ba", each_ba, mine, nb - 1, zsend, (zrecv, zrecv), modes)
    lines = Exchange(3, "ma", each_ma, me, n - 1, rsend, (rr0, rr_ref))

    loads[0].wait()
    loads[1].wait()
    for b in range(bl):
        both = dot(fv[...], jnp.concatenate([xv[b, h] for h in range(rows)], axis=1), (1, 1))
        re, im = both[:n * rows], both[n * rows:]
        for k in range(parts):
            csend[b * parts + k] = side(lane(re, k), lane(im, k)).astype(BF).reshape(n, rows, LANES)
        if b == 0:
            pl.semaphore_wait(barrier, n - 1 + nb - 1)
        cols.start(b)

    loads[3].wait()
    loads[8].wait()
    turned = sv[...].astype(F32).T.astype(BF)
    wide = jnp.broadcast_to(bv[...], (LANES, C)).T
    bias = jnp.concatenate([wide, wide], axis=1)
    for b in range(bl):
        for h in range(rows):
            (sk0, sk_ref)[b][:, h * W:(h + 1) * W] = dot(turned, xv[b, h]) + bias

    def rows_down(b):
        cols.wait_recv(b)
        col = jnp.concatenate([crecv[b * parts + k].reshape(n * rows, LANES) for k in range(parts)], axis=1)
        for k, v in enumerate(turn(dot(dv[...], col), 1.0)):
            ysend[b * parts + k] = v.astype(BF).reshape(nb, PAD, LANES)
        specs.start(b)

    def mix(b):
        specs.wait_recv(b)
        for k in range(parts):
            m1[k] = yrecv[b * parts + k].reshape(nb * PAD, LANES).astype(F32)
        for i in range(modes):
            at = pl.ds(i, nb, stride=PAD)
            v = [m1[k, at, :] for k in range(parts)]
            re, im = [jnp.concatenate([lane(a, p) for a in v], axis=1) for p in range(2)]
            a1 = jnp.concatenate([re, im], axis=0).astype(BF)
            a2 = jnp.concatenate([-im, re], axis=0).astype(BF)
            o = dot(a1, wv[0, i]) + dot(a2, wv[1, i])
            for k in range(parts):
                mo[k, at, :] = side(lane(o[:nb], k), lane(o[nb:], k))
        for k in range(parts):
            zsend[b * parts + k] = mo[k].astype(BF).reshape(nb, PAD, LANES)
        mixed.start(b)

    def rows_up(b):
        mixed.wait_recv(b)
        z = jnp.concatenate([zrecv[b * parts + k].reshape(nb * PAD, LANES) for k in range(parts)], axis=1)
        for k, v in enumerate(turn(dot(uv[...], z), -1.0)):
            rsend[b * parts + k] = v.astype(BF).reshape(n, rows, LANES)
        lines.start(b)

    loads[2].wait()
    rows_down(0)
    rows_down(1)
    loads[4].wait()
    loads[5].wait()
    mix(0)
    mix(1)
    loads[6].wait()
    rows_up(0)
    rows_up(1)
    loads[7].wait()
    for e in (cols, specs, mixed):
        for b in range(bl):
            e.wait_send(b)
    lines.wait_recv(0)
    rt = turned_lines([rr0[k].reshape(n * rows, LANES) for k in range(parts)])
    for h in range(rows):
        at = slice(h * W, (h + 1) * W)
        done_ref[h] = last_step(rt, lv_ref, at, sk0[:, at])
    lines.wait_recv(1)
    for b in range(bl):
        lines.wait_send(b)


def final_kernel(done_ref, rr_ref, sk_ref, lv_ref, out_ref, ov, sems):
    bl, rows, C, W = out_ref.shape
    parts = C // HALF
    copies = [pltpu.make_async_copy(done_ref, out_ref.at[0], sems.at[rows])]
    copies[0].start()
    rt = turned_lines([rr_ref[k].reshape(-1, LANES) for k in range(parts)])
    for h in range(rows):
        at = slice(h * W, (h + 1) * W)
        ov[h] = last_step(rt, lv_ref, at, sk_ref[:, at])
        c = pltpu.make_async_copy(ov.at[h], out_ref.at[1, h], sems.at[h])
        c.start()
        copies.append(c)
    for c in copies:
        c.wait()


def kernels(n, nb, H, KX, KY, fields, weight_real, weight_imag, skip_weight, out_bias):
    bl, rows, W, C = fields.shape
    modes = weight_real.shape[0]
    first, down, up, last = packed_tables(H, W, KX, KY, n, nb)
    fields = fields.transpose(0, 1, 3, 2)
    vmem = pl.BlockSpec(memory_space=pltpu.VMEM)
    hbm = pl.BlockSpec(memory_space=pltpu.HBM)
    parts = C // HALF
    half_block = (parts, n, rows, LANES)
    skip_block = (C, rows * W)
    ma_block = pltpu.VMEM((bl * parts, n, rows, LANES), BF)
    ba_block = pltpu.VMEM((bl * parts, nb, PAD, LANES), BF)
    mix_block = pltpu.VMEM((parts, nb * PAD, LANES), F32)
    dma = pltpu.SemaphoreType.DMA
    half = pl.pallas_call(
        functools.partial(spectral_kernel, n, nb),
        out_shape=(
            jax.ShapeDtypeStruct(fields.shape[1:], BF),
            jax.ShapeDtypeStruct(half_block, BF),
            jax.ShapeDtypeStruct(skip_block, F32),
            jax.ShapeDtypeStruct(last.shape, BF),
        ),
        in_specs=[hbm] * 9,
        out_specs=(vmem,) * 4,
        scratch_shapes=[
            pltpu.VMEM(fields.shape, BF), pltpu.VMEM(first.shape, BF), pltpu.VMEM(down.shape, BF),
            pltpu.VMEM(up.shape, BF), pltpu.VMEM((2, modes, C, C), BF), pltpu.VMEM((C, C), BF),
            pltpu.VMEM((1, C), F32), ma_block, ma_block, ba_block, ba_block, mix_block, mix_block,
            ba_block, ba_block, ma_block, pltpu.VMEM(half_block, BF), pltpu.VMEM(skip_block, F32),
            dma((9,)), dma((4, bl)), dma((4, bl)),
        ],
        compiler_params=pltpu.CompilerParams(
            collective_id=0, has_side_effects=True, vmem_limit_bytes=24 * 2**20
        ),
        name="spectral",
    )(*[
        pltpu.with_memory_space_constraint(a, pltpu.HBM)
        for a in (fields, weight_real, weight_imag, skip_weight, out_bias.reshape(1, C), first, down, up, last)
    ])
    out = pl.pallas_call(
        final_kernel,
        out_shape=jax.ShapeDtypeStruct(fields.shape, BF),
        in_specs=[vmem] * 4,
        out_specs=hbm,
        scratch_shapes=[pltpu.VMEM(fields.shape[1:], BF), dma((rows + 1,))],
        compiler_params=pltpu.CompilerParams(vmem_limit_bytes=16 * 2**20),
        name="finish",
    )(*half)
    return out.transpose(0, 1, 3, 2)


def solution(mesh):
    n, nb = mesh.shape["ma"], mesh.shape["ba"]

    def local(fields, weight_real, weight_imag, skip_weight, out_bias):
        sizes = (fields.shape[1] * n, weight_real.shape[0] * nb, weight_real.shape[1] * n)
        return kernels(n, nb, *sizes, fields, weight_real, weight_imag, skip_weight, out_bias)

    split = P("ba", "ma", None, None)
    return jax.shard_map(
        local, mesh=mesh, in_specs=(split, split, split, P(), P()), out_specs=split, check_vma=False
    )
```

```python
import functools
import math

import jax
import jax.numpy as jnp
import numpy as np
from jax import lax
from jax.experimental import pallas as pl
from jax.experimental.pallas import tpu as pltpu
from jax.sharding import PartitionSpec as P

MESH = pl.DeviceIdType.MESH
BF = jnp.bfloat16
F32 = jnp.float32
LANES = 128
HALF = 64
PAD = 16
PLAN = ((0, 0), (0, 1), (1, 0), (0, 2), (1, 1), (1, 2))
TURNS = (4, 5, 3, 6, 2, 7, 1)


def offsets():
    out = [
        (dz, dx, dc) for dc in (1, 0) for dxs in ((2,), (1, 3), (0,)) for dz in TURNS for dx in dxs
    ]
    return out + [(0, dx, dc) for dx, dc in ((2, 1), (2, 0), (1, 1), (3, 1), (1, 0), (3, 0), (0, 1))]


def ring(group):
    xs = ((2,), (1, 3), (0,))[group]
    out = [(dz, dx, dc) for dc in (1, 0) for dz in TURNS for dx in xs]
    if group == 2:
        out += [o for o in offsets() if o[0] == 0]
    return out


def hops(o):
    return min(o[0], 8 - o[0]) + min(o[1], 4 - o[1])


def angles(left, right, extent):
    turn = 2.0 * np.pi / extent * ((left[:, None] * right[None, :]) % extent)
    return np.cos(turn), np.sin(turn)


def packed_tables(H, W, KX, KY, n, nb):
    rows, modes = H // n, KX // nb
    s = 1.0 / math.sqrt(H * W)
    ky = np.arange(KY)
    eye = np.eye(rows)
    cos_w, sin_w = angles(ky, np.arange(W), W)
    g = np.where(ky == 0, 1.0, 2.0)[:, None] * s
    wide = []
    for f in (s, g):
        both = np.stack([cos_w * f, -sin_w * f], 0)
        wide.append(np.einsum("pkw,hg->pkhgw", both, eye).reshape(2 * KY * rows, rows * W))
    i = np.arange(KX)
    kx = np.where(i < KX // 2, i, i + H - KX)
    both = np.stack(angles(kx, np.arange(H), H), 0).reshape(2, nb, modes, H)
    both = np.pad(both, ((0, 0), (0, 0), (0, PAD - modes), (0, 0))).reshape(2, nb * PAD, H)
    down = both.reshape(2 * nb * PAD, H)
    up = both.transpose(0, 2, 1).reshape(2 * H, nb * PAD)
    return [jnp.asarray(a.astype(np.float32)).astype(BF) for a in (wide[0], down, up, wide[1])]


def dot(a, b, over=(1, 0)):
    return lax.dot_general(a, b, (((over[0],), (over[1],)), ((), ())), preferred_element_type=F32)


def lane(a, k):
    return a[:, k * HALF:(k + 1) * HALF]


def side(a, b):
    return jnp.concatenate([a, b], axis=1)


def turn(both, sign):
    m = both.shape[0] // 2
    low = lax.broadcasted_iota(jnp.int32, (m, LANES), 1) < HALF
    out = []
    for k in range(both.shape[1] // LANES):
        p, q = both[:m, k * LANES:(k + 1) * LANES], both[m:, k * LANES:(k + 1) * LANES]
        q = side(lane(q, 1), lane(q, 0))
        out.append(p + jnp.where(low, sign * q, -sign * q))
    return out


def turned_lines(parts):
    out = []
    for r in parts:
        t = r.astype(F32).T.astype(BF)
        out.append(side(t[:HALF], t[HALF:]))
    return jnp.concatenate(out, axis=0)


def last_step(rt, lv_ref, at, sk):
    v = dot(rt, lv_ref[:, at]) + sk
    c = math.sqrt(2.0 / math.pi)
    half = 0.5 * v
    return (half + half * jnp.tanh(v * (c + (0.044715 * c) * (v * v)))).astype(BF)


def spectral_kernel(
    n, nb, x_ref, wr_ref, wi_ref, skip_ref, bias_ref, first_ref, down_ref, up_ref, last_ref,
    done_ref, rr_ref, sk_ref, lv_ref,
    xv, fv, dv, uv, wv, sv, bv, csend, crecv, ysend, yrecv, m1, mo, zsend, zrecv, rsend, rr0, sk0,
    lsem, send_sem, recv_sem,
):
    bl, rows, C, W = x_ref.shape
    modes = wr_ref.shape[0]
    parts = C // HALF
    me = lax.axis_index("ma")
    mine = lax.axis_index("ba")
    az, ax, ac = me // 8, (me // 2) % 4, me % 2

    loads = [
        pltpu.make_async_copy(a, b, lsem.at[k]) for k, (a, b) in enumerate((
            (x_ref, xv), (first_ref, fv), (down_ref, dv), (skip_ref, sv),
            (wr_ref.at[:, 0], wv.at[0]), (wi_ref.at[:, 0], wv.at[1]), (up_ref, uv), (last_ref, lv_ref),
            (bias_ref, bv),
        ))
    ]
    for c in loads:
        c.start()

    def peer(dz, dx, dc):
        return (az + dz) % 8 * 8 + (ax + dx) % 4 * 2 + (ac + dc) % 2

    def each_ma(body, order=None):
        for o in order or offsets():
            body(peer(*o))

    def each_ba(body):
        for j in (4, 3, 5, 2, 6, 1, 7):
            body((mine + j) % nb)

    barrier = pltpu.get_barrier_semaphore()
    for o in sorted(offsets(), key=lambda o: -hops(o)):
        pl.semaphore_signal(barrier, inc=1, device_id={"ma": peer(*o)}, device_id_type=MESH)
    each_ba(lambda to: pl.semaphore_signal(barrier, inc=1, device_id={"ba": to}, device_id_type=MESH))

    zrecv[:, :, modes:, :] = jnp.zeros((bl * parts, nb, PAD - modes, LANES), BF)

    def group(ref, b):
        return ref if ref.shape[0] == parts else ref.at[parts * b:parts * (b + 1)]

    class Exchange:
        def __init__(self, kind, axis, each, here, count, send, recv, used=None):
            self.kind, self.axis, self.each, self.here, self.count = kind, axis, each, here, count
            self.send, self.recv, self.used = send, recv, used

        def block(self, ref, b, d):
            v = group(ref, b)
            return v.at[:, d] if self.used is None else v.at[:, d, 0:self.used]

        def start(self, b, *order):
            def go(to):
                pltpu.make_async_remote_copy(
                    src_ref=self.block(self.send, b, to), dst_ref=self.block(self.recv[b], b, self.here),
                    send_sem=send_sem.at[self.kind, b], recv_sem=recv_sem.at[self.kind, b],
                    device_id={self.axis: to}, device_id_type=MESH,
                ).start()

            self.each(go, *order)

        def keep(self, b):
            self.block(self.recv[b], b, self.here)[...] = self.block(self.send, b, self.here)[...]

        def wait(self, ref, b, sem):
            every = self.block(ref, b, slice(0, self.count))
            pltpu.make_async_copy(every, every, sem.at[self.kind, b]).wait()

        def wait_recv(self, b):
            self.wait(self.recv[b], b, recv_sem)

        def wait_send(self, b):
            self.wait(self.send, b, send_sem)

    cols = Exchange(0, "ma", each_ma, me, n - 1, csend, (crecv, crecv))
    specs = Exchange(1, "ba", each_ba, mine, nb - 1, ysend, (yrecv, yrecv), modes)
    mixed = Exchange(2, "ba", each_ba, mine, nb - 1, zsend, (zrecv, zrecv), modes)
    lines = Exchange(3, "ma", each_ma, me, n - 1, rsend, (rr0, rr_ref))

    loads[0].wait()
    loads[1].wait()
    for b in range(bl):
        both = dot(fv[...], jnp.concatenate([xv[b, h] for h in range(rows)], axis=1), (1, 1))
        re, im = both[:n * rows], both[n * rows:]
        for k in range(parts):
            csend[b * parts + k] = side(lane(re, k), lane(im, k)).astype(BF).reshape(n, rows, LANES)
    pl.semaphore_wait(barrier, n - 1 + nb - 1)
    for b, k in PLAN:
        cols.start(b, ring(k))
    for b in range(bl):
        cols.keep(b)

    loads[3].wait()
    loads[8].wait()
    turned = sv[...].astype(F32).T.astype(BF)
    wide = jnp.broadcast_to(bv[...], (LANES, C)).T
    bias = jnp.concatenate([wide, wide], axis=1)
    for b in range(bl):
        for h in range(rows):
            (sk0, sk_ref)[b][:, h * W:(h + 1) * W] = dot(turned, xv[b, h]) + bias

    def rows_down(b):
        cols.wait_recv(b)
        col = jnp.concatenate([crecv[b * parts + k].reshape(n * rows, LANES) for k in range(parts)], axis=1)
        for k, v in enumerate(turn(dot(dv[...], col), 1.0)):
            ysend[b * parts + k] = v.astype(BF).reshape(nb, PAD, LANES)
        specs.start(b)
        specs.keep(b)

    def mix(b):
        specs.wait_recv(b)
        for k in range(parts):
            m1[k] = yrecv[b * parts + k].reshape(nb * PAD, LANES).astype(F32)
        for i in range(modes):
            at = pl.ds(i, nb, stride=PAD)
            v = [m1[k, at, :] for k in range(parts)]
            re, im = [jnp.concatenate([lane(a, p) for a in v], axis=1) for p in range(2)]
            a1 = jnp.concatenate([re, im], axis=0).astype(BF)
            a2 = jnp.concatenate([-im, re], axis=0).astype(BF)
            o = dot(a1, wv[0, i]) + dot(a2, wv[1, i])
            for k in range(parts):
                mo[k, at, :] = side(lane(o[:nb], k), lane(o[nb:], k))
        for k in range(parts):
            zsend[b * parts + k] = mo[k].astype(BF).reshape(nb, PAD, LANES)
        mixed.start(b)
        mixed.keep(b)

    def rows_up(b):
        mixed.wait_recv(b)
        z = jnp.concatenate([zrecv[b * parts + k].reshape(nb * PAD, LANES) for k in range(parts)], axis=1)
        for k, v in enumerate(turn(dot(uv[...], z), -1.0)):
            rsend[b * parts + k] = v.astype(BF).reshape(n, rows, LANES)
        lines.start(b)
        lines.keep(b)

    loads[2].wait()
    rows_down(0)
    rows_down(1)
    loads[4].wait()
    loads[5].wait()
    mix(0)
    mix(1)
    loads[6].wait()
    rows_up(0)
    rows_up(1)
    loads[7].wait()
    for e in (cols, specs, mixed):
        for b in range(bl):
            e.wait_send(b)
    lines.wait_recv(0)
    rt = turned_lines([rr0[k].reshape(n * rows, LANES) for k in range(parts)])
    for h in range(rows):
        at = slice(h * W, (h + 1) * W)
        done_ref[h] = last_step(rt, lv_ref, at, sk0[:, at])
    lines.wait_recv(1)
    for b in range(bl):
        lines.wait_send(b)


def final_kernel(done_ref, rr_ref, sk_ref, lv_ref, out_ref, ov, sems):
    bl, rows, C, W = out_ref.shape
    parts = C // HALF
    copies = [pltpu.make_async_copy(done_ref, out_ref.at[0], sems.at[rows])]
    copies[0].start()
    rt = turned_lines([rr_ref[k].reshape(-1, LANES) for k in range(parts)])
    for h in range(rows):
        at = slice(h * W, (h + 1) * W)
        ov[h] = last_step(rt, lv_ref, at, sk_ref[:, at])
        c = pltpu.make_async_copy(ov.at[h], out_ref.at[1, h], sems.at[h])
        c.start()
        copies.append(c)
    for c in copies:
        c.wait()


def kernels(n, nb, H, KX, KY, fields, weight_real, weight_imag, skip_weight, out_bias):
    bl, rows, W, C = fields.shape
    modes = weight_real.shape[0]
    first, down, up, last = packed_tables(H, W, KX, KY, n, nb)
    fields = fields.transpose(0, 1, 3, 2)
    vmem = pl.BlockSpec(memory_space=pltpu.VMEM)
    hbm = pl.BlockSpec(memory_space=pltpu.HBM)
    parts = C // HALF
    half_block = (parts, n, rows, LANES)
    skip_block = (C, rows * W)
    ma_block = pltpu.VMEM((bl * parts, n, rows, LANES), BF)
    ba_block = pltpu.VMEM((bl * parts, nb, PAD, LANES), BF)
    mix_block = pltpu.VMEM((parts, nb * PAD, LANES), F32)
    dma = pltpu.SemaphoreType.DMA
    half = pl.pallas_call(
        functools.partial(spectral_kernel, n, nb),
        out_shape=(
            jax.ShapeDtypeStruct(fields.shape[1:], BF),
            jax.ShapeDtypeStruct(half_block, BF),
            jax.ShapeDtypeStruct(skip_block, F32),
            jax.ShapeDtypeStruct(last.shape, BF),
        ),
        in_specs=[hbm] * 9,
        out_specs=(vmem,) * 4,
        scratch_shapes=[
            pltpu.VMEM(fields.shape, BF), pltpu.VMEM(first.shape, BF), pltpu.VMEM(down.shape, BF),
            pltpu.VMEM(up.shape, BF), pltpu.VMEM((2, modes, C, C), BF), pltpu.VMEM((C, C), BF),
            pltpu.VMEM((1, C), F32), ma_block, ma_block, ba_block, ba_block, mix_block, mix_block,
            ba_block, ba_block, ma_block, pltpu.VMEM(half_block, BF), pltpu.VMEM(skip_block, F32),
            dma((9,)), dma((4, bl)), dma((4, bl)),
        ],
        compiler_params=pltpu.CompilerParams(
            collective_id=0, has_side_effects=True, vmem_limit_bytes=24 * 2**20
        ),
        name="spectral",
    )(*[
        pltpu.with_memory_space_constraint(a, pltpu.HBM)
        for a in (fields, weight_real, weight_imag, skip_weight, out_bias.reshape(1, C), first, down, up, last)
    ])
    out = pl.pallas_call(
        final_kernel,
        out_shape=jax.ShapeDtypeStruct(fields.shape, BF),
        in_specs=[vmem] * 4,
        out_specs=hbm,
        scratch_shapes=[pltpu.VMEM(fields.shape[1:], BF), dma((rows + 1,))],
        compiler_params=pltpu.CompilerParams(vmem_limit_bytes=16 * 2**20),
        name="finish",
    )(*half)
    return out.transpose(0, 1, 3, 2)


def solution(mesh):
    n, nb = mesh.shape["ma"], mesh.shape["ba"]

    def local(fields, weight_real, weight_imag, skip_weight, out_bias):
        sizes = (fields.shape[1] * n, weight_real.shape[0] * nb, weight_real.shape[1] * n)
        return kernels(n, nb, *sizes, fields, weight_real, weight_imag, skip_weight, out_bias)

    split = P("ba", "ma", None, None)
    return jax.shard_map(
        local, mesh=mesh, in_specs=(split, split, split, P(), P()), out_specs=split, check_vma=False
    )
```

```python
import functools
import math

import jax
import jax.numpy as jnp
import numpy as np
from jax import lax
from jax.experimental import pallas as pl
from jax.experimental.pallas import tpu as pltpu
from jax.sharding import PartitionSpec as P

MESH = pl.DeviceIdType.MESH
BF = jnp.bfloat16
F32 = jnp.float32
LANES = 128
HALF = 64
PAD = 16
PLAN = ((0, 0), (0, 1), (1, 0), (0, 2), (1, 1), (1, 2))
TURNS = (4, 3, 5, 2, 6, 1, 7)


def offsets():
    out = [
        (dz, dx, dc) for dc in (1, 0) for dxs in ((2,), (1, 3), (0,)) for dz in TURNS for dx in dxs
    ]
    return out + [(0, dx, dc) for dx, dc in ((2, 1), (2, 0), (1, 1), (3, 1), (1, 0), (3, 0), (0, 1))]


def ring(group):
    xs = ((2,), (1, 3), (0,))[group]
    out = [(dz, dx, dc) for dc in (1, 0) for dz in TURNS for dx in xs]
    if group == 2:
        out += [o for o in offsets() if o[0] == 0]
    return out


def hops(o):
    return min(o[0], 8 - o[0]) + min(o[1], 4 - o[1])


def angles(left, right, extent):
    turn = 2.0 * np.pi / extent * ((left[:, None] * right[None, :]) % extent)
    return np.cos(turn), np.sin(turn)


def packed_tables(H, W, KX, KY, n, nb):
    rows, modes = H // n, KX // nb
    s = 1.0 / math.sqrt(H * W)
    ky = np.arange(KY)
    eye = np.eye(rows)
    cos_w, sin_w = angles(ky, np.arange(W), W)
    g = np.where(ky == 0, 1.0, 2.0)[:, None] * s
    wide = []
    for f in (s, g):
        both = np.stack([cos_w * f, -sin_w * f], 0)
        wide.append(np.einsum("pkw,hg->pkhgw", both, eye).reshape(2 * KY * rows, rows * W))
    i = np.arange(KX)
    kx = np.where(i < KX // 2, i, i + H - KX)
    both = np.stack(angles(kx, np.arange(H), H), 0).reshape(2, nb, modes, H)
    both = np.pad(both, ((0, 0), (0, 0), (0, PAD - modes), (0, 0))).reshape(2, nb * PAD, H)
    down = both.reshape(2 * nb * PAD, H)
    up = both.transpose(0, 2, 1).reshape(2 * H, nb * PAD)
    return [jnp.asarray(a.astype(np.float32)).astype(BF) for a in (wide[0], down, up, wide[1])]


def dot(a, b, over=(1, 0)):
    return lax.dot_general(a, b, (((over[0],), (over[1],)), ((), ())), preferred_element_type=F32)


def lane(a, k):
    return a[:, k * HALF:(k + 1) * HALF]


def side(a, b):
    return jnp.concatenate([a, b], axis=1)


def turn(both, sign):
    m = both.shape[0] // 2
    low = lax.broadcasted_iota(jnp.int32, (m, LANES), 1) < HALF
    out = []
    for k in range(both.shape[1] // LANES):
        p, q = both[:m, k * LANES:(k + 1) * LANES], both[m:, k * LANES:(k + 1) * LANES]
        q = side(lane(q, 1), lane(q, 0))
        out.append(p + jnp.where(low, sign * q, -sign * q))
    return out


def turned_lines(parts):
    out = []
    for r in parts:
        t = r.astype(F32).T.astype(BF)
        out.append(side(t[:HALF], t[HALF:]))
    return jnp.concatenate(out, axis=0)


def last_step(rt, lv_ref, at, sk):
    v = dot(rt, lv_ref[:, at]) + sk
    c = math.sqrt(2.0 / math.pi)
    half = 0.5 * v
    return (half + half * jnp.tanh(v * (c + (0.044715 * c) * (v * v)))).astype(BF)


def spectral_kernel(
    n, nb, x_ref, wr_ref, wi_ref, skip_ref, bias_ref, first_ref, down_ref, up_ref, last_ref,
    done_ref, rr_ref, sk_ref, lv_ref,
    xv, fv, dv, uv, wv, sv, bv, csend, crecv, ysend, yrecv, m1, mo, zsend, zrecv, rsend, rr0, sk0,
    lsem, send_sem, recv_sem,
):
    bl, rows, C, W = x_ref.shape
    modes = wr_ref.shape[0]
    parts = C // HALF
    me = lax.axis_index("ma")
    mine = lax.axis_index("ba")
    az, ax, ac = me // 8, (me // 2) % 4, me % 2

    loads = [
        pltpu.make_async_copy(a, b, lsem.at[k]) for k, (a, b) in enumerate((
            (x_ref, xv), (first_ref, fv), (down_ref, dv), (skip_ref, sv),
            (wr_ref.at[:, 0], wv.at[0]), (wi_ref.at[:, 0], wv.at[1]), (up_ref, uv), (last_ref, lv_ref),
            (bias_ref, bv),
        ))
    ]
    for c in loads:
        c.start()

    def peer(dz, dx, dc):
        return (az + dz) % 8 * 8 + (ax + dx) % 4 * 2 + (ac + dc) % 2

    def each_ma(body, order=None):
        for o in order or offsets():
            body(peer(*o))

    def each_ba(body):
        for j in (4, 3, 5, 2, 6, 1, 7):
            body((mine + j) % nb)

    barrier = pltpu.get_barrier_semaphore()
    for o in sorted(offsets(), key=lambda o: -hops(o)):
        pl.semaphore_signal(barrier, inc=1, device_id={"ma": peer(*o)}, device_id_type=MESH)
    each_ba(lambda to: pl.semaphore_signal(barrier, inc=1, device_id={"ba": to}, device_id_type=MESH))

    zrecv[:, :, modes:, :] = jnp.zeros((bl * parts, nb, PAD - modes, LANES), BF)

    def group(ref, b):
        return ref if ref.shape[0] == parts else ref.at[parts * b:parts * (b + 1)]

    class Exchange:
        def __init__(self, kind, axis, each, here, count, send, recv, used=None):
            self.kind, self.axis, self.each, self.here, self.count = kind, axis, each, here, count
            self.send, self.recv, self.used = send, recv, used

        def block(self, ref, b, d):
            v = group(ref, b)
            return v.at[:, d] if self.used is None else v.at[:, d, 0:self.used]

        def start(self, b, *order):
            def go(to):
                pltpu.make_async_remote_copy(
                    src_ref=self.block(self.send, b, to), dst_ref=self.block(self.recv[b], b, self.here),
                    send_sem=send_sem.at[self.kind, b], recv_sem=recv_sem.at[self.kind, b],
                    device_id={self.axis: to}, device_id_type=MESH,
                ).start()

            self.each(go, *order)

        def keep(self, b):
            self.block(self.recv[b], b, self.here)[...] = self.block(self.send, b, self.here)[...]

        def wait(self, ref, b, sem):
            every = self.block(ref, b, slice(0, self.count))
            pltpu.make_async_copy(every, every, sem.at[self.kind, b]).wait()

        def wait_recv(self, b):
            self.wait(self.recv[b], b, recv_sem)

        def wait_send(self, b):
            self.wait(self.send, b, send_sem)

    cols = Exchange(0, "ma", each_ma, me, n - 1, csend, (crecv, crecv))
    specs = Exchange(1, "ba", each_ba, mine, nb - 1, ysend, (yrecv, yrecv), modes)
    mixed = Exchange(2, "ba", each_ba, mine, nb - 1, zsend, (zrecv, zrecv), modes)
    lines = Exchange(3, "ma", each_ma, me, n - 1, rsend, (rr0, rr_ref))

    loads[0].wait()
    loads[1].wait()
    for b in range(bl):
        both = dot(fv[...], jnp.concatenate([xv[b, h] for h in range(rows)], axis=1), (1, 1))
        re, im = both[:n * rows], both[n * rows:]
        for k in range(parts):
            csend[b * parts + k] = side(lane(re, k), lane(im, k)).astype(BF).reshape(n, rows, LANES)
    pl.semaphore_wait(barrier, n - 1 + nb - 1)
    for b, k in PLAN:
        cols.start(b, ring(k))
    for b in range(bl):
        cols.keep(b)

    loads[3].wait()
    loads[8].wait()
    turned = sv[...].astype(F32).T.astype(BF)
    wide = jnp.broadcast_to(bv[...], (LANES, C)).T
    bias = jnp.concatenate([wide, wide], axis=1)
    for b in range(bl):
        for h in range(rows):
            (sk0, sk_ref)[b][:, h * W:(h + 1) * W] = dot(turned, xv[b, h]) + bias

    def rows_down(b):
        cols.wait_recv(b)
        col = jnp.concatenate([crecv[b * parts + k].reshape(n * rows, LANES) for k in range(parts)], axis=1)
        for k, v in enumerate(turn(dot(dv[...], col), 1.0)):
            ysend[b * parts + k] = v.astype(BF).reshape(nb, PAD, LANES)
        specs.start(b)
        specs.keep(b)

    def mix(b):
        specs.wait_recv(b)
        for k in range(parts):
            m1[k] = yrecv[b * parts + k].reshape(nb * PAD, LANES).astype(F32)
        for i in range(modes):
            at = pl.ds(i, nb, stride=PAD)
            v = [m1[k, at, :] for k in range(parts)]
            re, im = [jnp.concatenate([lane(a, p) for a in v], axis=1) for p in range(2)]
            a1 = jnp.concatenate([re, im], axis=0).astype(BF)
            a2 = jnp.concatenate([-im, re], axis=0).astype(BF)
            o = dot(a1, wv[0, i]) + dot(a2, wv[1, i])
            for k in range(parts):
                mo[k, at, :] = side(lane(o[:nb], k), lane(o[nb:], k))
        for k in range(parts):
            zsend[b * parts + k] = mo[k].astype(BF).reshape(nb, PAD, LANES)
        mixed.start(b)
        mixed.keep(b)

    def rows_up(b):
        mixed.wait_recv(b)
        z = jnp.concatenate([zrecv[b * parts + k].reshape(nb * PAD, LANES) for k in range(parts)], axis=1)
        for k, v in enumerate(turn(dot(uv[...], z), -1.0)):
            rsend[b * parts + k] = v.astype(BF).reshape(n, rows, LANES)
        lines.start(b)
        lines.keep(b)

    loads[2].wait()
    rows_down(0)
    rows_down(1)
    loads[4].wait()
    loads[5].wait()
    mix(0)
    mix(1)
    loads[6].wait()
    rows_up(0)
    rows_up(1)
    loads[7].wait()
    for e in (cols, specs, mixed):
        for b in range(bl):
            e.wait_send(b)
    lines.wait_recv(0)
    rt = turned_lines([rr0[k].reshape(n * rows, LANES) for k in range(parts)])
    for h in range(rows):
        at = slice(h * W, (h + 1) * W)
        done_ref[h] = last_step(rt, lv_ref, at, sk0[:, at])
    lines.wait_recv(1)
    for b in range(bl):
        lines.wait_send(b)


def final_kernel(done_ref, rr_ref, sk_ref, lv_ref, out_ref, ov, sems):
    bl, rows, C, W = out_ref.shape
    parts = C // HALF
    copies = [pltpu.make_async_copy(done_ref, out_ref.at[0], sems.at[rows])]
    copies[0].start()
    rt = turned_lines([rr_ref[k].reshape(-1, LANES) for k in range(parts)])
    for h in range(rows):
        at = slice(h * W, (h + 1) * W)
        ov[h] = last_step(rt, lv_ref, at, sk_ref[:, at])
        c = pltpu.make_async_copy(ov.at[h], out_ref.at[1, h], sems.at[h])
        c.start()
        copies.append(c)
    for c in copies:
        c.wait()


def kernels(n, nb, H, KX, KY, fields, weight_real, weight_imag, skip_weight, out_bias):
    bl, rows, W, C = fields.shape
    modes = weight_real.shape[0]
    first, down, up, last = packed_tables(H, W, KX, KY, n, nb)
    fields = fields.transpose(0, 1, 3, 2)
    vmem = pl.BlockSpec(memory_space=pltpu.VMEM)
    hbm = pl.BlockSpec(memory_space=pltpu.HBM)
    parts = C // HALF
    half_block = (parts, n, rows, LANES)
    skip_block = (C, rows * W)
    ma_block = pltpu.VMEM((bl * parts, n, rows, LANES), BF)
    ba_block = pltpu.VMEM((bl * parts, nb, PAD, LANES), BF)
    mix_block = pltpu.VMEM((parts, nb * PAD, LANES), F32)
    dma = pltpu.SemaphoreType.DMA
    half = pl.pallas_call(
        functools.partial(spectral_kernel, n, nb),
        out_shape=(
            jax.ShapeDtypeStruct(fields.shape[1:], BF),
            jax.ShapeDtypeStruct(half_block, BF),
            jax.ShapeDtypeStruct(skip_block, F32),
            jax.ShapeDtypeStruct(last.shape, BF),
        ),
        in_specs=[hbm] * 9,
        out_specs=(vmem,) * 4,
        scratch_shapes=[
            pltpu.VMEM(fields.shape, BF), pltpu.VMEM(first.shape, BF), pltpu.VMEM(down.shape, BF),
            pltpu.VMEM(up.shape, BF), pltpu.VMEM((2, modes, C, C), BF), pltpu.VMEM((C, C), BF),
            pltpu.VMEM((1, C), F32), ma_block, ma_block, ba_block, ba_block, mix_block, mix_block,
            ba_block, ba_block, ma_block, pltpu.VMEM(half_block, BF), pltpu.VMEM(skip_block, F32),
            dma((9,)), dma((4, bl)), dma((4, bl)),
        ],
        compiler_params=pltpu.CompilerParams(
            collective_id=0, has_side_effects=True, vmem_limit_bytes=24 * 2**20
        ),
        name="spectral",
    )(*[
        pltpu.with_memory_space_constraint(a, pltpu.HBM)
        for a in (fields, weight_real, weight_imag, skip_weight, out_bias.reshape(1, C), first, down, up, last)
    ])
    out = pl.pallas_call(
        final_kernel,
        out_shape=jax.ShapeDtypeStruct(fields.shape, BF),
        in_specs=[vmem] * 4,
        out_specs=hbm,
        scratch_shapes=[pltpu.VMEM(fields.shape[1:], BF), dma((rows + 1,))],
        compiler_params=pltpu.CompilerParams(vmem_limit_bytes=16 * 2**20),
        name="finish",
    )(*half)
    return out.transpose(0, 1, 3, 2)


def solution(mesh):
    n, nb = mesh.shape["ma"], mesh.shape["ba"]

    def local(fields, weight_real, weight_imag, skip_weight, out_bias):
        sizes = (fields.shape[1] * n, weight_real.shape[0] * nb, weight_real.shape[1] * n)
        return kernels(n, nb, *sizes, fields, weight_real, weight_imag, skip_weight, out_bias)

    split = P("ba", "ma", None, None)
    return jax.shard_map(
        local, mesh=mesh, in_specs=(split, split, split, P(), P()), out_specs=split, check_vma=False
    )
```
